32 devices in a mesh: groups: 2 (over x), seq: 16 (over z, y, core).
Axes of the slice: x: 2, y: 2, z: 4, core: 2. Of those that a mesh axis runs over, the one named last changes fastest.
Arguments:
- queries: bfloat16 [8192, 4096], P(('groups', 'seq')), parts along dimension 0, may hold values from -13 to 13
- keys: bfloat16 [8192, 512], P(('groups', 'seq')), parts along dimension 0, may hold values from -13 to 13
- values: bfloat16 [8192, 512], P(('groups', 'seq')), parts along dimension 0, may hold values from -6 to 6
- segment_ids: int32 [8192], P(('groups', 'seq')), parts along dimension 0, may hold values from 0 to 8, as said below
Outputs:
- attended: bfloat16 [8192, 4096], P(('groups', 'seq')), parts along dimension 0
- rotated_keys: bfloat16 [8192, 512], P(('groups', 'seq')), parts along dimension 0
The draws below stay inside these ranges and needn't reach their ends.
There are 2 independent parts, one for each index of `groups`. The reference program is written for one: setup_inputs(seed, part) draws one part's arguments, and reference() takes and returns one part's arrays. A program takes and returns all parts, laid end to end along the dimension named above; each array names one. Nothing has to cross between parts.
Inputs may be any that keep to these rules, and one draw needn't show every extreme that they name: `segment_ids`: never falling along the packed stream, starting at 0 and rising by one at each new rollout; each rollout covers 1 to 1792 tokens and one covers exactly 1792.
All inputs are finite; a program needn't handle non-finite values.
Results may differ from the reference program's by a relative error of at most 0.0054.
Values may be sent and summed in bfloat16 or wider, within the bound.
A program may use at most 192 MiB of HBM per device.

```python
import jax
import jax.numpy as jnp
from jax import lax

HQ = 32
HK = 4
HD = 128
SPAN = 7
TOK_DEV = 256
TOKENS = 4096
N_SEQ = 16


def base_draw(own_key, width):
    return jnp.clip(jax.random.normal(own_key, (TOKENS, width), jnp.float32), -6.0, 6.0)


def draw_queries(key, part):
    drawn = base_draw(jax.random.fold_in(key, 21), HQ * HD)
    return drawn.astype(jnp.bfloat16)


def draw_keys(key, part):
    drawn = base_draw(jax.random.fold_in(key, 22), HK * HD)
    return drawn.astype(jnp.bfloat16)


def draw_segment_ids(key, part):
    quarter = TOK_DEV // 4
    offset_key = jax.random.fold_in(key, 31)
    lead_offset = jax.random.randint(jax.random.fold_in(offset_key, 1), (), 1, quarter)
    first_cut = (N_SEQ // 2 - 1) * TOK_DEV + jax.random.randint(jax.random.fold_in(offset_key, 2), (), 1, TOK_DEV)
    second_cut = N_SEQ // 2 * TOK_DEV + jax.random.randint(jax.random.fold_in(offset_key, 3), (), 1, TOK_DEV)
    third_cut = (N_SEQ // 2 + 1) * TOK_DEV + jax.random.randint(jax.random.fold_in(offset_key, 4), (), 1, TOK_DEV)
    window_count = N_SEQ // 2
    window_number = jnp.arange(window_count, dtype=jnp.int32)
    window_shift = jax.random.randint(jax.random.fold_in(offset_key, 5), (window_count,), 0, TOK_DEV)
    window_place = window_number * (2 * TOK_DEV) + window_shift
    window_used = (window_number >= 4) & (window_number != N_SEQ // 4 - 1) & (window_number != N_SEQ // 4)
    window_place = jnp.where(window_used, window_place, 0)
    marks = jnp.zeros((TOKENS,), jnp.int32)
    marks = marks.at[window_place].max(window_used.astype(jnp.int32))
    marks = marks.at[0].set(1)
    marks = marks.at[lead_offset].set(1)
    marks = marks.at[lead_offset + SPAN * TOK_DEV].set(1)
    marks = marks.at[first_cut].set(1)
    marks = marks.at[second_cut].set(1)
    marks = marks.at[third_cut].set(1)
    return (jnp.cumsum(marks) - 1).astype(jnp.int32)


def shard_levels(key, shape, shards, smallest, top_value):
    def one(axis_at, blocks):
        heights = jax.random.uniform(jax.random.fold_in(jax.random.fold_in(key, 6), axis_at), (blocks,), jnp.float32, smallest / len(shards), top_value / len(shards))
        return jnp.repeat(jnp.exp(heights), shape[axis_at] // blocks).reshape((-1,) + (1,) * (len(shape) - axis_at - 1))

    loudness = one(*shards[0])
    for cut in shards[1:]:
        loudness = loudness * one(*cut)
    return loudness


def gaussian(rng, shape, deviation, most, split=(), kind=jnp.bfloat16):
    entries = deviation * jax.random.normal(rng, shape, jnp.float32)
    if split:
        entries = entries * shard_levels(rng, shape, split, -0.22, 0.18)
    return jnp.clip(entries, -most, most).astype(kind)


def setup_inputs(seed: int = 0, part: int = 0) -> dict:
    splits = jax.random.split(jax.random.key(seed), 5)
    part_splits = jax.random.split(jax.random.fold_in(splits[4], part), 5)
    queries = draw_queries(jax.random.fold_in(jax.random.fold_in(splits[4], part), 71), part)
    keys = draw_keys(jax.random.fold_in(jax.random.fold_in(splits[4], part), 71), part)
    values = gaussian(part_splits[2], (TOKENS, HK * HD), 1.0, 6.0, ((0, 16),))
    segment_ids = draw_segment_ids(jax.random.fold_in(jax.random.fold_in(splits[4], part), 71), part)
    return dict(queries=queries, keys=keys, values=values, segment_ids=segment_ids)


ROPE_BASE = 1000000.0
MASKED_SCORE = -1.0e30


def rollout_starts(segment_ids):
    token_index = jnp.arange(segment_ids.shape[0], dtype=jnp.int32)
    boundary = jnp.concatenate([jnp.ones((1,), dtype=jnp.bool_), segment_ids[1:] != segment_ids[:-1]])
    return lax.cummax(jnp.where(boundary, token_index, -1), axis=0)


def rotate_heads(matrix, positions, head_count):
    row_count = matrix.shape[0]
    half_dim = HD // 2
    inverse_freq = ROPE_BASE ** (-(jnp.arange(half_dim, dtype=jnp.float32) * (2.0 / HD)))
    angles = positions.astype(jnp.float32)[:, None] * inverse_freq[None, :]
    cosine = jnp.cos(angles)[:, None, :]
    sine = jnp.sin(angles)[:, None, :]
    split_heads = matrix.astype(jnp.float32).reshape(row_count, head_count, HD)
    lower_half = split_heads[..., :half_dim]
    upper_half = split_heads[..., half_dim:]
    turned = jnp.concatenate([lower_half * cosine - upper_half * sine, upper_half * cosine + lower_half * sine], axis=-1)
    return turned.reshape(row_count, head_count * HD).astype(jnp.bfloat16)


def reference(queries, keys, values, segment_ids):
    token_count = queries.shape[0]
    starts = rollout_starts(segment_ids)
    positions = jnp.arange(token_count, dtype=jnp.int32) - starts
    turned_queries = rotate_heads(queries, positions, HQ)
    rotated_keys = rotate_heads(keys, positions, HK)
    reach_rows = SPAN * TOK_DEV
    window_rows = (SPAN + 1) * TOK_DEV
    group_size = HQ // HK
    padded_keys = jnp.concatenate([jnp.zeros((reach_rows, HK * HD), jnp.bfloat16), rotated_keys], axis=0)
    padded_values = jnp.concatenate([jnp.zeros((reach_rows, HK * HD), jnp.bfloat16), values], axis=0)

    def one_block(block_number):
        block_first = (block_number * TOK_DEV).astype(jnp.int32)
        query_block = lax.dynamic_slice_in_dim(turned_queries, block_first, TOK_DEV, 0).astype(jnp.float32).reshape(TOK_DEV, HK, group_size, HD)
        key_window = lax.dynamic_slice_in_dim(padded_keys, block_first, window_rows, 0).astype(jnp.float32).reshape(window_rows, HK, HD)
        value_window = lax.dynamic_slice_in_dim(padded_values, block_first, window_rows, 0).astype(jnp.float32).reshape(window_rows, HK, HD)
        query_starts = lax.dynamic_slice_in_dim(starts, block_first, TOK_DEV, 0)
        query_index = block_first + jnp.arange(TOK_DEV, dtype=jnp.int32)
        key_index = block_first - reach_rows + jnp.arange(window_rows, dtype=jnp.int32)
        allowed = (key_index[None, :] >= query_starts[:, None]) & (key_index[None, :] <= query_index[:, None])
        scores = jnp.einsum("thgd,shd->thgs", query_block, key_window) * (HD ** -0.5)
        scores = jnp.where(allowed[:, None, None, :], scores, MASKED_SCORE)
        row_top = jnp.max(scores, axis=-1, keepdims=True)
        weights = jnp.exp(scores - row_top)
        totals = jnp.sum(weights, axis=-1, keepdims=True)
        rounded_weights = lax.optimization_barrier(weights.astype(jnp.bfloat16)).astype(jnp.float32)
        mixed = jnp.einsum("thgs,shd->thgd", rounded_weights, value_window) / totals
        return mixed.reshape(TOK_DEV, HQ * HD).astype(jnp.bfloat16)

    attended = lax.map(one_block, jnp.arange(N_SEQ, dtype=jnp.int32))
    return (attended.reshape(token_count, HQ * HD), rotated_keys)
```

```python
from functools import partial

import jax
import jax.numpy as jnp
from jax import lax
from jax.experimental import pallas as pl
from jax.experimental.pallas import tpu as pltpu
from jax.sharding import PartitionSpec as P

HD = 128
SPAN = 7
ROPE_BASE = 1000000.0
BIG = 1e30
NO_SEGMENT = 127
LANES = 128
ONES_ROWS = 16


def shifted(shard, axis, by):
    length = lax.axis_size(axis)
    pairs = [(i, i + by) for i in range(length) if 0 <= i + by < length]
    return lax.ppermute(shard, axis, pairs)


def tables(positions):
    half_dim = HD // 2
    inverse_freq = ROPE_BASE ** (-(jnp.arange(half_dim, dtype=jnp.float32) * (2.0 / HD)))
    angles = positions.astype(jnp.float32)[:, None] * inverse_freq[None, :]
    cosine, sine = jnp.cos(angles), jnp.sin(angles)
    return (
        jnp.concatenate([cosine, cosine], axis=-1),
        jnp.concatenate([-sine, sine], axis=-1),
    )


def rotate_heads(matrix, cosine, sine):
    rows, width = matrix.shape
    heads = matrix.astype(jnp.float32).reshape(rows, width // HD, HD)
    swapped = jnp.concatenate([heads[..., HD // 2 :], heads[..., : HD // 2]], axis=-1)
    turned = heads * cosine[:, None, :] + swapped * sine[:, None, :]
    return turned.reshape(rows, width).astype(jnp.bfloat16)


def one_hot(segment_row):
    rows = lax.broadcasted_iota(jnp.int32, (LANES, segment_row.shape[1]), 0)
    return jnp.where(rows == segment_row, 1.0, 0.0).T


def attend_phase(slots, head, group, qa, qhot, k_ref, khot, vt, top, acc, causal):
    first = causal is not None
    query = jnp.concatenate([qa[head], qhot[...]], axis=1)
    kv = head // group
    columns = pl.ds(pl.multiple_of(kv * HD, HD), HD)
    parts = []
    for slot in slots:
        key = jnp.concatenate([k_ref[slot, :, columns], khot[slot]], axis=1)
        part = lax.dot_general(
            key, query, (((1,), (1,)), ((), ())), preferred_element_type=jnp.float32
        )
        parts.append(part + causal[...] if first else part)
    new_top = jnp.max(parts[0], axis=0, keepdims=True)
    for part in parts[1:]:
        new_top = jnp.maximum(new_top, jnp.max(part, axis=0, keepdims=True))
    if not first:
        old_top = top[head]
        new_top = jnp.maximum(new_top, old_top)
    mixed = None
    for slot, part in zip(slots, parts):
        weights = jnp.exp2(part - new_top).astype(jnp.bfloat16)
        term = jnp.dot(vt[slot, kv], weights, preferred_element_type=jnp.float32)
        mixed = term if mixed is None else mixed + term
    if not first:
        mixed = mixed + acc[head] * jnp.exp2(old_top - new_top)
    return new_top, mixed


def kernel(
    group, phases, q_ref, cos_ref, sin_ref, k_ref, v_ref, seg_ref, out_ref,
    qa, qhot, khot, vt, top, acc, causal,
):
    rows = q_ref.shape[0]
    heads = q_ref.shape[1] // HD
    kv_heads = heads // group
    count = k_ref.shape[0]
    scale = HD ** (-0.5) * 1.4426950408889634
    cosine = cos_ref[...] * scale
    sine = sin_ref[...] * scale

    def turn(head, carry):
        columns = pl.ds(pl.multiple_of(head * HD, HD), HD)
        x = q_ref[:, columns].astype(jnp.float32)
        qa[head] = (x * cosine + pltpu.roll(x, HD // 2, 1) * sine).astype(jnp.bfloat16)
        return carry

    lax.fori_loop(0, heads, turn, 0)
    qhot[...] = ((one_hot(seg_ref[0]) - 1.0) * BIG).astype(jnp.bfloat16)
    key_at = lax.broadcasted_iota(jnp.int32, (rows, rows), 0)
    query_at = lax.broadcasted_iota(jnp.int32, (rows, rows), 1)
    causal[...] = jnp.where(key_at <= query_at, 0.0, -BIG)

    def prepare(slot, carry):
        khot[slot] = one_hot(seg_ref[slot]).astype(jnp.bfloat16)
        for kv in range(kv_heads):
            vt[slot, kv, :HD, :] = (
                v_ref[slot, :, kv * HD : (kv + 1) * HD].astype(jnp.float32).T.astype(jnp.bfloat16)
            )
            vt[slot, kv, HD:, :] = jnp.ones((ONES_ROWS, rows), jnp.bfloat16)
        return carry

    lax.fori_loop(0, count, prepare, 0)
    for number, slots in enumerate(phases):
        last = number == len(phases) - 1

        def step(index, carry):
            for head in (2 * index, 2 * index + 1):
                new_top, mixed = attend_phase(
                    slots, head, group, qa, qhot, k_ref, khot, vt, top, acc,
                    causal if number == 0 else None,
                )
                if last:
                    columns = pl.ds(pl.multiple_of(head * HD, HD), HD)
                    result = mixed[:HD] * (1.0 / mixed[HD : HD + 1])
                    out_ref[:, columns] = result.T.astype(jnp.bfloat16)
                else:
                    top[head] = new_top
                    acc[head] = mixed
            return carry

        lax.fori_loop(0, heads // 2, step, 0)


def local(queries, keys, values, segment_ids):
    block_rows = queries.shape[0]
    query_heads = queries.shape[1] // HD
    kv_heads = keys.shape[1] // HD
    group = query_heads // kv_heads
    my_rank = lax.axis_index("seq")
    row_index = my_rank * block_rows + jnp.arange(block_rows, dtype=jnp.int32)
    cosine, sine = tables(row_index)
    key_stack = rotate_heads(keys, cosine, sine)[None]
    value_stack = values[None]
    seg_stack = segment_ids[None, None]
    for stride_bit in range((SPAN + 1).bit_length() - 1):
        far = shifted((key_stack, value_stack, seg_stack), "seq", 1 << stride_bit)
        key_stack = jnp.concatenate([key_stack, far[0]], axis=0)
        value_stack = jnp.concatenate([value_stack, far[1]], axis=0)
        seg_stack = jnp.concatenate([seg_stack, far[2]], axis=0)
    count = key_stack.shape[0]
    present = jnp.arange(count) <= my_rank
    seg_stack = jnp.where(present[:, None, None], seg_stack, NO_SEGMENT)
    vmem = pl.BlockSpec(memory_space=pltpu.VMEM)
    attended = pl.pallas_call(
        partial(kernel, group, ((0,), (1, 2, 3, 4), (5, 6, 7))),
        out_shape=jax.ShapeDtypeStruct(queries.shape, jnp.bfloat16),
        in_specs=[vmem] * 6,
        out_specs=vmem,
        scratch_shapes=[
            pltpu.VMEM((query_heads, block_rows, HD), jnp.bfloat16),
            pltpu.VMEM((block_rows, LANES), jnp.bfloat16),
            pltpu.VMEM((count, block_rows, LANES), jnp.bfloat16),
            pltpu.VMEM((count, kv_heads, HD + ONES_ROWS, block_rows), jnp.bfloat16),
            pltpu.VMEM((query_heads, 1, block_rows), jnp.float32),
            pltpu.VMEM((query_heads, HD + ONES_ROWS, block_rows), jnp.float32),
            pltpu.VMEM((block_rows, block_rows), jnp.float32),
        ],
        compiler_params=pltpu.CompilerParams(vmem_limit_bytes=60 * 1024 * 1024),
    )(queries, cosine, sine, key_stack, value_stack, seg_stack)

    boundary = jnp.concatenate(
        [jnp.ones((1,), dtype=jnp.bool_), segment_ids[1:] != segment_ids[:-1]]
    )
    local_start = lax.cummax(jnp.where(boundary, row_index, -1), axis=0)
    earlier = jnp.sum((seg_stack[1:] == segment_ids[0]).astype(jnp.int32))
    starts = jnp.where(
        segment_ids == segment_ids[0], my_rank * block_rows - earlier, local_start
    )
    turned_keys = rotate_heads(keys, *tables(row_index - starts))
    return (attended, turned_keys)


def solution(mesh):
    in_specs = (
        P(("groups", "seq"), None),
        P(("groups", "seq"), None),
        P(("groups", "seq"), None),
        P(("groups", "seq")),
    )
    out_specs = (P(("groups", "seq"), None), P(("groups", "seq"), None))
    return jax.shard_map(local, mesh=mesh, in_specs=in_specs, out_specs=out_specs, check_vma=False)
```

```python
from functools import partial

import jax
import jax.numpy as jnp
from jax import lax
from jax.experimental import pallas as pl
from jax.experimental.pallas import tpu as pltpu
from jax.sharding import PartitionSpec as P

HD = 128
SPAN = 7
ROPE_BASE = 1000000.0
BIG = 1e30
NO_SEGMENT = 127
LANES = 128
ONES_ROWS = 16
SEG_ROWS = 16
PIECES = 4


def tables(positions):
    half_dim = HD // 2
    inverse_freq = ROPE_BASE ** (-(jnp.arange(half_dim, dtype=jnp.float32) * (2.0 / HD)))
    angles = positions.astype(jnp.float32)[:, None] * inverse_freq[None, :]
    cosine, sine = jnp.cos(angles), jnp.sin(angles)
    return (
        jnp.concatenate([cosine, cosine], axis=-1),
        jnp.concatenate([-sine, sine], axis=-1),
    )


def rotate_heads(matrix, cosine, sine):
    rows, width = matrix.shape
    heads = matrix.astype(jnp.float32).reshape(rows, width // HD, HD)
    swapped = jnp.concatenate([heads[..., HD // 2 :], heads[..., : HD // 2]], axis=-1)
    turned = heads * cosine[:, None, :] + swapped * sine[:, None, :]
    return turned.reshape(rows, width).astype(jnp.bfloat16)


def one_hot(segment_row):
    rows = lax.broadcasted_iota(jnp.int32, (LANES, segment_row.shape[1]), 0).astype(jnp.float32)
    return jnp.where(rows == segment_row, 1.0, 0.0).T


def attend_phase(slots, head, group, qa, qhot, block, khot, vt, top, acc, causal):
    first = causal is not None
    rows = qhot.shape[0]
    query = jnp.concatenate([qa[head], qhot[...]], axis=1)
    kv = head // group
    at = pl.ds(pl.multiple_of(SEG_ROWS + kv * rows, SEG_ROWS), rows)
    parts = []
    for slot in slots:
        key = jnp.concatenate([block(slot)[at, :HD], khot[slot]], axis=1)
        part = lax.dot_general(
            key, query, (((1,), (1,)), ((), ())), preferred_element_type=jnp.float32
        )
        parts.append(part + causal[...] if first else part)
    new_top = jnp.max(parts[0], axis=0, keepdims=True)
    for part in parts[1:]:
        new_top = jnp.maximum(new_top, jnp.max(part, axis=0, keepdims=True))
    if not first:
        old_top = top[head]
        new_top = jnp.maximum(new_top, old_top)
    mixed = None
    for slot, part in zip(slots, parts):
        weights = jnp.exp2(part - new_top).astype(jnp.bfloat16)
        term = jnp.dot(vt[slot, kv], weights, preferred_element_type=jnp.float32)
        mixed = term if mixed is None else mixed + term
    if not first:
        mixed = mixed + acc[head] * jnp.exp2(old_top - new_top)
    return new_top, mixed


def kernel(
    group, count, q_ref, cos_ref, sin_ref, own_ref, keys_ref, freq_ref, out_ref, rot_ref,
    recv, qa, qhot, khot, vt, top, acc, causal, send_sems, recv_sems,
):
    rows = q_ref.shape[0]
    heads = q_ref.shape[1] // HD
    kv_heads = heads // group
    me = lax.axis_index("seq")
    core = lax.rem(me, 2)
    side = lax.rem(me // 2, 2)
    plane = me // 4
    planes = count // 4
    partner = me + 1 - 2 * core
    across = me + 2 - 4 * side
    ahead = me + 4
    behind = me - 4
    has_ahead = plane + 1 < planes
    has_behind = plane >= 1

    def block(slot):
        return own_ref if slot == 0 else recv.at[slot]

    def chunk(piece):
        if piece == 0:
            return pl.ds(0, SEG_ROWS + rows)
        return pl.ds(SEG_ROWS + piece * rows, rows)

    barrier = pltpu.get_barrier_semaphore()

    def greet(device):
        pl.semaphore_signal(
            barrier, inc=1, device_id={"seq": device}, device_id_type=pl.DeviceIdType.MESH
        )

    greet(partner)
    greet(across)

    @pl.when(has_ahead)
    def _():
        greet(ahead)

    @pl.when(has_behind)
    def _():
        greet(behind)

    both = has_ahead & has_behind
    one = (has_ahead | has_behind) & jnp.logical_not(both)
    neither = jnp.logical_not(has_ahead | has_behind)
    for extra, condition in ((2, both), (1, one), (0, neither)):

        @pl.when(condition)
        def _():
            pl.semaphore_wait(barrier, 2 + extra)

    sent = []

    def copy(kind, piece, source, distance, device):
        src = own_ref if source is None else recv.at[source]
        return pltpu.make_async_remote_copy(
            src_ref=src.at[chunk(piece)],
            dst_ref=recv.at[distance, chunk(piece)],
            send_sem=send_sems.at[kind, piece],
            recv_sem=recv_sems.at[distance, piece],
            device_id={"seq": device},
            device_id_type=pl.DeviceIdType.MESH,
        )

    def send(condition, *what):
        @pl.when(condition)
        def _():
            copy(*what).start()

        sent.append((condition, what))

    def arrive(condition, distance, piece):
        @pl.when(condition)
        def _():
            copy(0, piece, None, distance, partner).wait_recv()

    to_partner = 1 - 2 * core
    has_two = (side == 1) | (plane >= 1)
    has_six = ((side == 1) & (plane >= 1)) | (plane >= 2)
    relays = (side == 1) | (core == 1)
    has_eight = (plane >= 2) & relays
    for piece in range(PIECES):
        send(has_ahead, 0, piece, None, 4, ahead)
        send(side == 0, 1, piece, None, 2, across)
        send(core == 0, 2, piece, None, 1, partner)

    def near(point):
        if point < PIECES:
            arrive(has_behind, 4, point)
            send(has_behind, 3, point, 4, 6 - 4 * side, across)
            send(has_behind & has_ahead & relays, 4, point, 4, 8, ahead)
            send(has_behind, 5, point, 4, 4 + to_partner, partner)
        if point > 0:
            arrive(has_two, 2, point - 1)
            send(has_two, 6, point - 1, 2, 2 + to_partner, partner)

    def far(point):
        if point < PIECES:
            arrive(has_eight, 8, point)
            send(has_eight & (side == 1), 7, point, 8, 6, across)
            send(has_eight & (core == 1), 8, point, 8, 7, partner)
        if point > 0:
            arrive(has_six, 6, point - 1)
            send(has_six, 9, point - 1, 6, 6 + to_partner, partner)

    filler = jnp.full((SEG_ROWS, 2 * HD), NO_SEGMENT, jnp.bfloat16)
    for distance in range(1, SPAN + 1):

        @pl.when(me < distance)
        def _():
            recv[distance, :SEG_ROWS, :] = filler
            recv[distance, SEG_ROWS:, :] = jnp.zeros((kv_heads * rows, 2 * HD), jnp.bfloat16)

    scale = HD ** (-0.5) * 1.4426950408889634
    cosine = cos_ref[...] * scale
    sine = sin_ref[...] * scale

    def turn(head, carry):
        columns = pl.ds(pl.multiple_of(head * HD, HD), HD)
        x = q_ref[:, columns].astype(jnp.float32)
        qa[head] = (x * cosine + pltpu.roll(x, HD // 2, 1) * sine).astype(jnp.bfloat16)
        return carry

    lax.fori_loop(0, heads, turn, 0)

    def segment_row(slot):
        return block(slot)[:SEG_ROWS, :].astype(jnp.float32)[:1]

    qhot[...] = ((one_hot(segment_row(0)) - 1.0) * BIG).astype(jnp.bfloat16)
    key_at = lax.broadcasted_iota(jnp.int32, (rows, rows), 0)
    query_at = lax.broadcasted_iota(jnp.int32, (rows, rows), 1)
    causal[...] = jnp.where(key_at <= query_at, 0.0, -BIG)

    def prepare(slots):
        for slot in slots:
            khot[slot] = one_hot(segment_row(slot)).astype(jnp.bfloat16)

            def flip(kv, carry):
                at = pl.ds(pl.multiple_of(SEG_ROWS + kv * rows, SEG_ROWS), rows)
                flipped = block(slot)[at, HD:].astype(jnp.float32).T
                vt[slot, kv, :HD, :] = flipped.astype(jnp.bfloat16)
                vt[slot, kv, HD:, :] = jnp.ones((ONES_ROWS, rows), jnp.bfloat16)
                return carry

            lax.fori_loop(0, kv_heads, flip, 0)

    def attend(slots, low, high, first, last):
        def step(index, carry):
            for head in (2 * index, 2 * index + 1):
                new_top, mixed = attend_phase(
                    slots, head, group, qa, qhot, block, khot, vt, top, acc,
                    causal if first else None,
                )
                if last:
                    columns = pl.ds(pl.multiple_of(head * HD, HD), HD)
                    result = mixed[:HD] * (1.0 / mixed[HD : HD + 1])
                    out_ref[:, columns] = result.T.astype(jnp.bfloat16)
                else:
                    top[head] = new_top
                    acc[head] = mixed
            return carry

        lax.fori_loop(low // 2, high // 2, step, 0)

    part = heads // PIECES
    prepare((0,))
    for piece in range(PIECES):
        near(piece)
        attend((0,), piece * part, (piece + 1) * part, True, False)
    near(PIECES)
    for piece in range(PIECES):
        arrive(me >= 1, 1, piece)
        arrive(me >= 3, 3, piece)
    prepare((1, 2, 3, 4))
    for piece in range(PIECES):
        far(piece)
        attend((1, 2, 3, 4), piece * part, (piece + 1) * part, False, False)
    far(PIECES)
    for piece in range(PIECES):
        arrive(me >= 5, 5, piece)
        arrive(me >= 7, 7, piece)
    prepare((5, 6, 7))
    attend((5, 6, 7), 0, heads, False, True)

    mine = segment_row(0)
    lead = mine[:, :1]
    earlier = jnp.zeros((1, 1), jnp.float32)
    for distance in range(1, SPAN + 1):
        same = jnp.where(segment_row(distance) == lead, 1.0, 0.0)
        earlier = earlier + jnp.sum(same, axis=1, keepdims=True)
    column = jnp.broadcast_to(mine, (LANES, rows)).T[:, :1]
    before = jnp.sum(jnp.where(mine < column, 1.0, 0.0), axis=1, keepdims=True)
    index = lax.broadcasted_iota(jnp.int32, (rows, 1), 0).astype(jnp.float32)
    positions = index - before + jnp.where(column == lead, earlier, 0.0)
    angles = positions * freq_ref[...]
    lane = lax.broadcasted_iota(jnp.int32, (rows, HD), 1)
    cosine = jnp.cos(angles)
    sine = jnp.where(lane < HD // 2, -1.0, 1.0) * jnp.sin(angles)
    for kv in range(kv_heads):
        x = keys_ref[:, kv * HD : (kv + 1) * HD].astype(jnp.float32)
        turned = x * cosine + pltpu.roll(x, HD // 2, 1) * sine
        rot_ref[:, kv * HD : (kv + 1) * HD] = turned.astype(jnp.bfloat16)

    for condition, what in sent:

        @pl.when(condition)
        def _():
            copy(*what).wait_send()


def local(queries, keys, values, segment_ids):
    rows = queries.shape[0]
    heads = queries.shape[1] // HD
    kv_heads = keys.shape[1] // HD
    count = lax.axis_size("seq")
    row_index = lax.axis_index("seq") * rows + jnp.arange(rows, dtype=jnp.int32)
    cosine, sine = tables(row_index)
    turned = rotate_heads(keys, cosine, sine)
    segment_rows = jnp.broadcast_to(segment_ids.astype(jnp.bfloat16)[None], (SEG_ROWS, rows))
    pieces = [segment_rows]
    for kv in range(kv_heads):
        part = slice(kv * HD, (kv + 1) * HD)
        pieces.append(jnp.concatenate([turned[:, part], values[:, part]], axis=1))
    own = jnp.concatenate(pieces, axis=0)
    inverse_freq = ROPE_BASE ** (-(jnp.arange(HD // 2, dtype=jnp.float32) * (2.0 / HD)))
    frequencies = jnp.concatenate([inverse_freq, inverse_freq])[None]
    vmem = pl.BlockSpec(memory_space=pltpu.VMEM)
    slots = SPAN + 2
    return pl.pallas_call(
        partial(kernel, heads // kv_heads, count),
        out_shape=(
            jax.ShapeDtypeStruct(queries.shape, jnp.bfloat16),
            jax.ShapeDtypeStruct(keys.shape, jnp.bfloat16),
        ),
        in_specs=[vmem] * 6,
        out_specs=(vmem, vmem),
        scratch_shapes=[
            pltpu.VMEM((slots, *own.shape), jnp.bfloat16),
            pltpu.VMEM((heads, rows, HD), jnp.bfloat16),
            pltpu.VMEM((rows, LANES), jnp.bfloat16),
            pltpu.VMEM((slots, rows, LANES), jnp.bfloat16),
            pltpu.VMEM((slots, kv_heads, HD + ONES_ROWS, rows), jnp.bfloat16),
            pltpu.VMEM((heads, 1, rows), jnp.float32),
            pltpu.VMEM((heads, HD + ONES_ROWS, rows), jnp.float32),
            pltpu.VMEM((rows, rows), jnp.float32),
            pltpu.SemaphoreType.DMA((10, PIECES)),
            pltpu.SemaphoreType.DMA((slots, PIECES)),
        ],
        compiler_params=pltpu.CompilerParams(
            vmem_limit_bytes=60 * 1024 * 1024, collective_id=0, has_side_effects=True
        ),
    )(queries, cosine, sine, own, keys, frequencies)


def solution(mesh):
    in_specs = (
        P(("groups", "seq"), None),
        P(("groups", "seq"), None),
        P(("groups", "seq"), None),
        P(("groups", "seq")),
    )
    out_specs = (P(("groups", "seq"), None), P(("groups", "seq"), None))
    return jax.shard_map(local, mesh=mesh, in_specs=in_specs, out_specs=out_specs, check_vma=False)
```

```python
from functools import partial

import jax
import jax.numpy as jnp
from jax import lax
from jax.experimental import pallas as pl
from jax.experimental.pallas import tpu as pltpu
from jax.sharding import PartitionSpec as P

HD = 128
SPAN = 7
ROPE_BASE = 1000000.0
BIG = 1e30
NO_SEGMENT = 127
LANES = 128
ONES_ROWS = 16
SEG_ROWS = 16
PIECES = 4


def tables(positions):
    half_dim = HD // 2
    inverse_freq = ROPE_BASE ** (-(jnp.arange(half_dim, dtype=jnp.float32) * (2.0 / HD)))
    angles = positions.astype(jnp.float32)[:, None] * inverse_freq[None, :]
    cosine, sine = jnp.cos(angles), jnp.sin(angles)
    return (
        jnp.concatenate([cosine, cosine], axis=-1),
        jnp.concatenate([-sine, sine], axis=-1),
    )


def rotate_heads(matrix, cosine, sine):
    rows, width = matrix.shape
    heads = matrix.astype(jnp.float32).reshape(rows, width // HD, HD)
    swapped = jnp.concatenate([heads[..., HD // 2 :], heads[..., : HD // 2]], axis=-1)
    turned = heads * cosine[:, None, :] + swapped * sine[:, None, :]
    return turned.reshape(rows, width).astype(jnp.bfloat16)


def one_hot(segment_row):
    rows = lax.broadcasted_iota(jnp.int32, (LANES, segment_row.shape[1]), 0).astype(jnp.float32)
    return jnp.where(rows == segment_row, 1.0, 0.0).T


def attend_phase(slots, head, group, qa, qhot, block, khot, vt, top, acc, causal):
    first = causal is not None
    rows = qhot.shape[0]
    query = jnp.concatenate([qa[head], qhot[...]], axis=1)
    kv = head // group
    at = pl.ds(pl.multiple_of(SEG_ROWS + kv * rows, SEG_ROWS), rows)
    keys = jnp.concatenate(
        [jnp.concatenate([block(slot)[at, :HD], khot[slot]], axis=1) for slot in slots], axis=0
    )
    scores = lax.dot_general(
        keys, query, (((1,), (1,)), ((), ())), preferred_element_type=jnp.float32
    )
    if first:
        scores = scores + causal[...]
    new_top = jnp.max(scores, axis=0, keepdims=True)
    if not first:
        old_top = top[head]
        new_top = jnp.maximum(new_top, old_top)
    weights = jnp.exp2(scores - new_top).astype(jnp.bfloat16)
    flipped = vt[kv, :, slots[0] * rows : (slots[-1] + 1) * rows]
    mixed = jnp.dot(flipped, weights, preferred_element_type=jnp.float32)
    if not first:
        mixed = mixed + acc[head] * jnp.exp2(old_top - new_top)
    return new_top, mixed


def kernel(
    group, count, q_ref, cos_ref, sin_ref, own_ref, keys_ref, freq_ref, out_ref, rot_ref,
    recv, qa, qhot, khot, vt, top, acc, causal, send_sems, recv_sems,
):
    rows = q_ref.shape[0]
    heads = q_ref.shape[1] // HD
    kv_heads = heads // group
    me = lax.axis_index("seq")
    core = lax.rem(me, 2)
    side = lax.rem(me // 2, 2)
    plane = me // 4
    planes = count // 4
    partner = me + 1 - 2 * core
    across = me + 2 - 4 * side
    ahead = me + 4
    behind = me - 4
    has_ahead = plane + 1 < planes
    has_behind = plane >= 1

    def block(slot):
        return own_ref if slot == 0 else recv.at[slot]

    def chunk(piece):
        if piece == 0:
            return pl.ds(0, SEG_ROWS + rows)
        return pl.ds(SEG_ROWS + piece * rows, rows)

    barrier = pltpu.get_barrier_semaphore()

    def greet(device):
        pl.semaphore_signal(
            barrier, inc=1, device_id={"seq": device}, device_id_type=pl.DeviceIdType.MESH
        )

    greet(partner)
    greet(across)

    @pl.when(has_ahead)
    def _():
        greet(ahead)

    @pl.when(has_behind)
    def _():
        greet(behind)

    both = has_ahead & has_behind
    one = (has_ahead | has_behind) & jnp.logical_not(both)
    neither = jnp.logical_not(has_ahead | has_behind)
    for extra, condition in ((2, both), (1, one), (0, neither)):

        @pl.when(condition)
        def _():
            pl.semaphore_wait(barrier, 2 + extra)

    sent = []

    def copy(kind, piece, source, distance, device):
        src = own_ref if source is None else recv.at[source]
        return pltpu.make_async_remote_copy(
            src_ref=src.at[chunk(piece)],
            dst_ref=recv.at[distance, chunk(piece)],
            send_sem=send_sems.at[kind, piece],
            recv_sem=recv_sems.at[distance, piece],
            device_id={"seq": device},
            device_id_type=pl.DeviceIdType.MESH,
        )

    def send(condition, *what):
        @pl.when(condition)
        def _():
            copy(*what).start()

        sent.append((condition, what))

    def arrive(condition, distance, piece):
        @pl.when(condition)
        def _():
            copy(0, piece, None, distance, partner).wait_recv()

    to_partner = 1 - 2 * core
    has_two = (side == 1) | (plane >= 1)
    has_six = ((side == 1) & (plane >= 1)) | (plane >= 2)
    relays = (side == 1) | (core == 1)
    has_eight = (plane >= 2) & relays
    for piece in range(PIECES):
        send(has_ahead, 0, piece, None, 4, ahead)
        send(side == 0, 1, piece, None, 2, across)
        send(core == 0, 2, piece, None, 1, partner)

    def near(point):
        if point < PIECES:
            arrive(has_behind, 4, point)
            send(has_behind, 3, point, 4, 6 - 4 * side, across)
            send(has_behind & has_ahead & relays, 4, point, 4, 8, ahead)
            send(has_behind, 5, point, 4, 4 + to_partner, partner)
        if point > 0:
            arrive(has_two, 2, point - 1)
            send(has_two, 6, point - 1, 2, 2 + to_partner, partner)

    def far(point):
        if point < PIECES:
            arrive(has_eight, 8, point)
            send(has_eight & (side == 1), 7, point, 8, 6, across)
            send(has_eight & (core == 1), 8, point, 8, 7, partner)
        if point > 0:
            arrive(has_six, 6, point - 1)
            send(has_six, 9, point - 1, 6, 6 + to_partner, partner)

    filler = jnp.full((SEG_ROWS, 2 * HD), NO_SEGMENT, jnp.bfloat16)
    for distance in range(1, SPAN + 1):

        @pl.when(me < distance)
        def _():
            recv[distance, :SEG_ROWS, :] = filler
            recv[distance, SEG_ROWS:, :] = jnp.zeros((kv_heads * rows, 2 * HD), jnp.bfloat16)

    scale = HD ** (-0.5) * 1.4426950408889634
    cosine = cos_ref[...] * scale
    sine = sin_ref[...] * scale

    def turn(head, carry):
        columns = pl.ds(pl.multiple_of(head * HD, HD), HD)
        x = q_ref[:, columns].astype(jnp.float32)
        qa[head] = (x * cosine + pltpu.roll(x, HD // 2, 1) * sine).astype(jnp.bfloat16)
        return carry

    lax.fori_loop(0, heads, turn, 0)

    def segment_row(slot):
        return block(slot)[:SEG_ROWS, :].astype(jnp.float32)[:1]

    qhot[...] = ((one_hot(segment_row(0)) - 1.0) * BIG).astype(jnp.bfloat16)
    key_at = lax.broadcasted_iota(jnp.int32, (rows, rows), 0)
    query_at = lax.broadcasted_iota(jnp.int32, (rows, rows), 1)
    causal[...] = jnp.where(key_at <= query_at, 0.0, -BIG)

    def prepare(slots):
        for slot in slots:
            khot[slot] = one_hot(segment_row(slot)).astype(jnp.bfloat16)

            def flip(kv, carry):
                at = pl.ds(pl.multiple_of(SEG_ROWS + kv * rows, SEG_ROWS), rows)
                flipped = block(slot)[at, HD:].astype(jnp.float32).T
                span = slice(slot * rows, (slot + 1) * rows)
                vt[kv, :HD, span] = flipped.astype(jnp.bfloat16)
                vt[kv, HD:, span] = jnp.ones((ONES_ROWS, rows), jnp.bfloat16)
                return carry

            lax.fori_loop(0, kv_heads, flip, 0)

    def attend(slots, low, high, first, last):
        def step(index, carry):
            for head in (2 * index, 2 * index + 1):
                new_top, mixed = attend_phase(
                    slots, head, group, qa, qhot, block, khot, vt, top, acc,
                    causal if first else None,
                )
                if last:
                    columns = pl.ds(pl.multiple_of(head * HD, HD), HD)
                    result = mixed[:HD] * (1.0 / mixed[HD : HD + 1])
                    out_ref[:, columns] = result.T.astype(jnp.bfloat16)
                else:
                    top[head] = new_top
                    acc[head] = mixed
            return carry

        lax.fori_loop(low // 2, high // 2, step, 0)

    part = heads // PIECES
    prepare((0,))
    for piece in range(PIECES):
        near(piece)
        attend((0,), piece * part, (piece + 1) * part, True, False)
    near(PIECES)
    for piece in range(PIECES):
        arrive(me >= 1, 1, piece)
        arrive(me >= 3, 3, piece)
    prepare((1, 2, 3, 4))
    for piece in range(PIECES):
        far(piece)
        attend((1, 2, 3, 4), piece * part, (piece + 1) * part, False, False)
    far(PIECES)
    for piece in range(PIECES):
        arrive(me >= 5, 5, piece)
        arrive(me >= 7, 7, piece)
    prepare((5, 6, 7))
    attend((5, 6, 7), 0, heads, False, True)

    mine = segment_row(0)
    lead = mine[:, :1]
    earlier = jnp.zeros((1, 1), jnp.float32)
    for distance in range(1, SPAN + 1):
        same = jnp.where(segment_row(distance) == lead, 1.0, 0.0)
        earlier = earlier + jnp.sum(same, axis=1, keepdims=True)
    column = jnp.broadcast_to(mine, (LANES, rows)).T[:, :1]
    before = jnp.sum(jnp.where(mine < column, 1.0, 0.0), axis=1, keepdims=True)
    index = lax.broadcasted_iota(jnp.int32, (rows, 1), 0).astype(jnp.float32)
    positions = index - before + jnp.where(column == lead, earlier, 0.0)
    angles = positions * freq_ref[...]
    lane = lax.broadcasted_iota(jnp.int32, (rows, HD), 1)
    cosine = jnp.cos(angles)
    sine = jnp.where(lane < HD // 2, -1.0, 1.0) * jnp.sin(angles)
    for kv in range(kv_heads):
        x = keys_ref[:, kv * HD : (kv + 1) * HD].astype(jnp.float32)
        turned = x * cosine + pltpu.roll(x, HD // 2, 1) * sine
        rot_ref[:, kv * HD : (kv + 1) * HD] = turned.astype(jnp.bfloat16)

    for condition, what in sent:

        @pl.when(condition)
        def _():
            copy(*what).wait_send()


def local(queries, keys, values, segment_ids):
    rows = queries.shape[0]
    heads = queries.shape[1] // HD
    kv_heads = keys.shape[1] // HD
    count = lax.axis_size("seq")
    row_index = lax.axis_index("seq") * rows + jnp.arange(rows, dtype=jnp.int32)
    cosine, sine = tables(row_index)
    turned = rotate_heads(keys, cosine, sine)
    segment_rows = jnp.broadcast_to(segment_ids.astype(jnp.bfloat16)[None], (SEG_ROWS, rows))
    pieces = [segment_rows]
    for kv in range(kv_heads):
        part = slice(kv * HD, (kv + 1) * HD)
        pieces.append(jnp.concatenate([turned[:, part], values[:, part]], axis=1))
    own = jnp.concatenate(pieces, axis=0)
    inverse_freq = ROPE_BASE ** (-(jnp.arange(HD // 2, dtype=jnp.float32) * (2.0 / HD)))
    frequencies = jnp.concatenate([inverse_freq, inverse_freq])[None]
    vmem = pl.BlockSpec(memory_space=pltpu.VMEM)
    slots = SPAN + 2
    return pl.pallas_call(
        partial(kernel, heads // kv_heads, count),
        out_shape=(
            jax.ShapeDtypeStruct(queries.shape, jnp.bfloat16),
            jax.ShapeDtypeStruct(keys.shape, jnp.bfloat16),
        ),
        in_specs=[vmem] * 6,
        out_specs=(vmem, vmem),
        scratch_shapes=[
            pltpu.VMEM((slots, *own.shape), jnp.bfloat16),
            pltpu.VMEM((heads, rows, HD), jnp.bfloat16),
            pltpu.VMEM((rows, LANES), jnp.bfloat16),
            pltpu.VMEM((slots, rows, LANES), jnp.bfloat16),
            pltpu.VMEM((kv_heads, HD + ONES_ROWS, slots * rows), jnp.bfloat16),
            pltpu.VMEM((heads, 1, rows), jnp.float32),
            pltpu.VMEM((heads, HD + ONES_ROWS, rows), jnp.float32),
            pltpu.VMEM((rows, rows), jnp.float32),
            pltpu.SemaphoreType.DMA((10, PIECES)),
            pltpu.SemaphoreType.DMA((slots, PIECES)),
        ],
        compiler_params=pltpu.CompilerParams(
            vmem_limit_bytes=60 * 1024 * 1024, collective_id=0, has_side_effects=True
        ),
    )(queries, cosine, sine, own, keys, frequencies)


def solution(mesh):
    in_specs = (
        P(("groups", "seq"), None),
        P(("groups", "seq"), None),
        P(("groups", "seq"), None),
        P(("groups", "seq")),
    )
    out_specs = (P(("groups", "seq"), None), P(("groups", "seq"), None))
    return jax.shard_map(local, mesh=mesh, in_specs=in_specs, out_specs=out_specs, check_vma=False)
```
